512 devices in a mesh: dp: 2 (over x_hi), seq: 8 (over y), tensor: 32 (over z, x_lo, core).
Axes of the slice: x: 4 (x_hi: 2, x_lo: 2; x = x_hi * 2 + x_lo), y: 8, z: 8, core: 2. Of those that a mesh axis runs over, the one named last changes fastest.
Arguments:
- activations: bfloat16 [4, 1536, 28672], P('dp', 'seq', 'tensor'), may hold values from -6 to 6
- gradients: bfloat16 [4, 1536, 8192], P('dp', 'seq', 'tensor'), may hold values from -6 to 6
- basis_in: bfloat16 [28672, 2048], P('tensor', 'seq'), may hold values from -0.03125 to 0.03125
- basis_out: bfloat16 [8192, 768], P('tensor', 'seq'), may hold values from -0.0625 to 0.0625
Outputs:
- corrected: float32 [2048, 768], P(('seq', 'tensor'))
The draws below stay inside these ranges and needn't reach their ends.
All inputs are finite; a program needn't handle non-finite values.
Results may differ from the reference program's by a relative error of at most 0.0034.
Values may be sent and summed in bfloat16 or wider, within the bound.
No kernel may reach another device: no remote copies, remote signals or barrier semaphores. Data moves between devices by JAX's collectives and lax.ppermute only.
A program may use at most 64 MiB of HBM per device.

```python
import jax
import jax.numpy as jnp

A = 28672
G = 8192
KG = 768
SEQS = 4
LEN = 1536
KA = 2048


def shard_levels(own_key, extent, split, low, high):
    gain, own = 1.0, jax.random.fold_in(own_key, 6)
    for position, parts in split:
        draws = jnp.exp(jax.random.uniform(jax.random.fold_in(own, position), (parts,), jnp.float32, low / len(split), high / len(split)))
        gain = gain * jnp.repeat(draws, extent[position] // parts).reshape([-1 if axis == position else 1 for axis in range(len(extent))])
    return gain


def normal_values(rng, extent, width, most, cuts=(), kind=jnp.bfloat16):
    drawn = width * jax.random.normal(rng, extent, jnp.float32)
    if cuts:
        drawn = drawn * shard_levels(rng, extent, cuts, -0.22, 0.18)
    return jnp.clip(drawn, -most, most).astype(kind)


def setup_inputs(seed: int = 0) -> dict:
    keys = jax.random.split(jax.random.key(seed), 5)
    return {
        "activations": normal_values(keys[0], (SEQS, LEN, A), 1.0, 6.0, ((0, 2), (1, 8), (2, 32))),
        "gradients": normal_values(keys[1], (SEQS, LEN, G), 1.0, 6.0, ((0, 2), (1, 8), (2, 32))),
        "basis_in": normal_values(keys[2], (A, KA), A ** -0.5, 0.03125, ((0, 32), (1, 8))),
        "basis_out": normal_values(keys[3], (G, KG), G ** -0.5, 0.0625, ((0, 32), (1, 8))),
    }


def reference(activations, gradients, basis_in, basis_out):
    act_rows = activations.reshape(SEQS * LEN, A)
    grad_rows = gradients.reshape(SEQS * LEN, G)
    projected_act = jnp.dot(act_rows, basis_in, preferred_element_type=jnp.float32).astype(jnp.bfloat16)
    projected_grad = jnp.dot(grad_rows, basis_out, preferred_element_type=jnp.float32).astype(jnp.bfloat16)
    projected_act = projected_act.reshape(SEQS, LEN, KA).astype(jnp.float32)
    projected_grad = projected_grad.reshape(SEQS, LEN, KG).astype(jnp.float32)
    blocks = jnp.einsum("stk,stj->skj", projected_act, projected_grad)
    corrected = jnp.sum(blocks * blocks, axis=0) / (SEQS * LEN)
    return corrected
```

```python
import jax
import jax.numpy as jnp
from jax import lax
from jax.experimental.layout import Layout, with_layout_constraint
from jax.sharding import Mesh
from jax.sharding import PartitionSpec as P

TENSOR = ("z", "x", "c")
SEQ_TENSOR = ("seq", "z", "x", "c")
ALL = ("dp", "seq", "z", "x", "c")
F32 = jnp.float32
BF16 = jnp.bfloat16


def exchange(v, axis):
    return lax.ppermute(v, axis, [(0, 1), (1, 0)])


def all_to_all(v, axis):
    return lax.all_to_all(v, axis, 0, 0, tiled=True)


def to_everyone(v, axis):
    return all_to_all(jnp.broadcast_to(v[None], (lax.axis_size(axis), *v.shape)), axis)


def from_offset(v, k):
    return lax.ppermute(v, "seq", [((i + k) % 8, i) for i in range(8)])


def contract_last(a, b):
    return lax.dot_general(
        a, b, (((a.ndim - 1,), (b.ndim - 1,)), ((), ())), preferred_element_type=F32
    )


def placements(sizes, same):
    pairs = []
    dps, seqs, zs, xs, cs = sizes

    def flat(d, y, z, x, c):
        return (((d * seqs + y) * zs + z) * xs + x) * cs + c

    def owner(row):
        t = row // 8
        return t // (xs * cs), t // cs % xs, t % cs

    for d in range(dps):
        for y in range(seqs):
            for z in range(zs):
                for x in range(xs):
                    for c in range(cs):
                        of = d if y // 4 == 0 else 1 - d
                        row = y % 4 * 8 + x * 32 + c * 64
                        to = d if same else 1 - d
                        pairs.append(
                            (flat(d, y, z, x, c), flat(to, z, *owner(of * 128 + row)))
                        )
    return pairs


def body(sizes, activations, gradients, basis_in, basis_out):
    d = lax.axis_index("dp")
    c = lax.axis_index("c")
    seqs, length, width = activations.shape
    tokens = seqs * length
    x_own = activations.reshape(tokens, width)
    g_own = gradients.reshape(tokens, -1)

    halves = basis_out.T.reshape(1, 2, -1, basis_out.shape[0])
    out_cols = all_to_all(
        jnp.broadcast_to(halves, (8, *halves.shape[1:])).reshape(16, -1, basis_out.shape[0]),
        ("seq", "c"),
    ).reshape(8, 2, -1, basis_out.shape[0])
    g_other = exchange(g_own, "c")

    half = lax.dynamic_slice_in_dim(basis_in, d * 128, 128, 1).T
    half = with_layout_constraint(half, Layout(major_to_minor=(0, 1)))
    mine = lax.dynamic_slice_in_dim(half, c * 64, 64, 0)
    theirs = lax.dynamic_slice_in_dim(half, (1 - c) * 64, 64, 0)
    block = jnp.concatenate([mine, exchange(theirs, "c")], 1)
    block = with_layout_constraint(block, Layout(major_to_minor=(0, 1)))
    up1, down1 = from_offset(block, 1), from_offset(block, -1)
    up2, down2 = from_offset(block, 2), from_offset(block, -2)
    up3, down3 = from_offset(up2, 1), from_offset(down2, -1)
    across = jnp.concatenate([from_offset(up2[:32], 2), from_offset(down2[32:], -2)], 0)
    blocks_in = [block, up1, up2, up3, across, down3, down2, down1]

    x_rows = jnp.concatenate([x_own, exchange(x_own, "dp")], 0)
    x_rows = jnp.concatenate([x_rows, exchange(x_rows, "c")], 1)

    first = jnp.where(c == 0, g_own, g_other)
    second = jnp.where(c == 0, g_other, g_own)
    width_out = out_cols.shape[0] * out_cols.shape[2]
    grad_partial = contract_last(out_cols[:, 0].reshape(width_out, -1), first) + contract_last(
        out_cols[:, 1].reshape(width_out, -1), second
    )
    grad_own = all_to_all(grad_partial.reshape(16, -1, tokens), ("z", "x")).sum(0).astype(BF16)
    grad_half = to_everyone(grad_own, ("z", "x")).reshape(8, -1, tokens)
    grad_rest = exchange(grad_half, "c")
    grads = jnp.where(
        c == 0,
        jnp.stack([grad_half, grad_rest], 1),
        jnp.stack([grad_rest, grad_half], 1),
    ).reshape(-1, tokens)

    part = jnp.stack([contract_last(k, x_rows).astype(BF16) for k in blocks_in])
    part = jnp.roll(part, lax.axis_index("seq"), 0).reshape(16, 32, -1)
    act = all_to_all(part, ("z", "x")).astype(F32).sum(0).astype(BF16)
    act = jnp.concatenate([act[:, :tokens], exchange(act[:, tokens:], "dp")], 0)

    of_seq = lax.broadcasted_iota(jnp.int32, (seqs, 1, tokens), 2) // length
    chosen = of_seq == lax.broadcasted_iota(jnp.int32, (seqs, 1, tokens), 0)
    masked = jnp.where(chosen, act[None], jnp.zeros((), BF16))
    partial_blocks = contract_last(masked, grads)
    pieces = partial_blocks.reshape(seqs, 8, 8, -1).swapaxes(0, 1)
    blocks = all_to_all(pieces, "seq").sum(0)
    squared = jnp.sum(blocks * blocks, axis=0)
    near = lax.ppermute(squared, ALL, placements(sizes, True))
    far = lax.ppermute(squared, ALL, placements(sizes, False))
    return (near + far) / (2 * seqs * 8 * length)


def solution(mesh):
    finer = Mesh(mesh.devices.reshape(2, 8, 8, 2, 2), ALL)
    sizes = finer.devices.shape
    in_specs = (P("dp", "seq", TENSOR), P("dp", "seq", TENSOR), P(TENSOR, "seq"), P(TENSOR, "seq"))
    out_specs = P(SEQ_TENSOR, None)

    def local(*args):
        return body(sizes, *args)

    return jax.shard_map(local, mesh=finer, in_specs=in_specs, out_specs=out_specs, check_vma=False)
```

```python
import jax
import jax.numpy as jnp
from jax import lax
from jax.experimental.layout import Layout, with_layout_constraint
from jax.sharding import Mesh
from jax.sharding import PartitionSpec as P


TENSOR = ("z", "x", "c")
SEQ_TENSOR = ("seq", "z", "x", "c")
ALL = ("dp", "seq", "z", "x", "c")
F32 = jnp.float32
BF16 = jnp.bfloat16


def exchange(v, axis):
    return lax.ppermute(v, axis, [(0, 1), (1, 0)])


def all_to_all(v, axis):
    return lax.all_to_all(v, axis, 0, 0, tiled=True)


def to_everyone(v, axis):
    return all_to_all(jnp.broadcast_to(v[None], (lax.axis_size(axis), *v.shape)), axis)


def contract_last(a, b):
    return lax.dot_general(
        a, b, (((a.ndim - 1,), (b.ndim - 1,)), ((), ())), preferred_element_type=F32
    )


def contract(a, b):
    return lax.dot_general(a, b, (((1,), (0,)), ((), ())), preferred_element_type=F32)


def seq_order(y):
    shape = (8, 8, 2, 4, 8)
    shard, row, core, slot, at = (lax.broadcasted_iota(jnp.int32, shape, k) for k in range(5))
    away = jnp.where(slot == 3, 4 * core, (slot + 1) * (2 * core - 1))
    picked = ((y + away - shard) % 8 == 0) & (row == at)
    return picked.astype(BF16).reshape(64, 64)


def ring_step(v, cores):
    n = lax.axis_size("seq")
    pairs = [(y * 2 + k, (y + 1 - 2 * k) % n * 2 + k) for y in range(n) for k in cores]
    return lax.ppermute(v, ("seq", "c"), pairs)


def to_core_of_dp(v):
    near = lax.ppermute(v, ("dp", "c"), [(d * 2 + c, c * 2 + d) for d in (0, 1) for c in (0, 1)])
    far = lax.ppermute(
        v, ("dp", "c"), [(d * 2 + c, (1 - c) * 2 + d) for d in (0, 1) for c in (0, 1)]
    )
    return near, far


def body(activations, gradients, basis_in, basis_out):
    d = lax.axis_index("dp")
    c = lax.axis_index("c")
    y = lax.axis_index("seq")
    seqs, length, width = activations.shape
    tokens = seqs * length
    x_own = activations.reshape(tokens, width)
    g_own = gradients.reshape(tokens, -1)

    x_far = exchange(x_own, "dp")

    halves = basis_out.T.reshape(1, 2, -1, basis_out.shape[0])
    spread = jnp.broadcast_to(halves, (8, *halves.shape[1:])).reshape(16, -1, basis_out.shape[0])
    out_cols = all_to_all(spread, ("seq", "c"))
    out_cols = out_cols.reshape(8, 2, -1, basis_out.shape[0])

    shard = with_layout_constraint(basis_in.T, Layout(major_to_minor=(0, 1)))
    half = shard.reshape(16, 2, 8, width)
    half = lax.dynamic_index_in_dim(half, d, 1, keepdims=False).reshape(128, width)
    partner = exchange(half, "c")
    g_other = exchange(g_own, "c")
    block = jnp.concatenate([half, partner], 1)
    step1 = ring_step(block, (0, 1))
    step2 = ring_step(step1, (0, 1))
    step3 = ring_step(step2, (0, 1))
    step4 = ring_step(step3, (1,))

    first = jnp.where(c == 0, g_own, g_other)
    second = jnp.where(c == 0, g_other, g_own)
    width_out = out_cols.shape[0] * out_cols.shape[2]
    grad_partial = contract_last(out_cols[:, 0].reshape(width_out, -1), first) + contract_last(
        out_cols[:, 1].reshape(width_out, -1), second
    )
    grad_parts = all_to_all(grad_partial.reshape(16, -1, tokens), ("z", "x"))
    grad_own = grad_parts.sum(0).astype(BF16)
    grad_half = to_everyone(grad_own, ("z", "x")).reshape(8, -1, tokens)
    near, far = to_core_of_dp(grad_half)
    grads = jnp.where(d == 0, jnp.stack([near, far], 1), jnp.stack([far, near], 1))
    grads = grads.reshape(-1, tokens)

    x_rows = jnp.where(
        d == 0, jnp.concatenate([x_own, x_far], 0), jnp.concatenate([x_far, x_own], 0)
    )
    x_other = exchange(x_rows, "c")
    x_rows = lax.optimization_barrier(jnp.concatenate([x_rows, x_other], 1))
    last = jnp.where(c == 0, block, step4)
    parts = [
        contract_last(k, x_rows).astype(BF16).reshape(16, 8, -1)
        for k in (step1, step2, step3, last)
    ]
    arrived = all_to_all(jnp.stack(parts, 1).reshape(16, 32, -1), ("z", "x"))
    act = arrived.astype(F32).sum(0).astype(BF16)

    left, right = act[:, :tokens], act[:, tokens:]
    mine = jnp.where(c == 0, left, right)
    theirs = exchange(jnp.where(c == 0, right, left), "c")
    zero = jnp.where(c == 0, mine, theirs)
    one = jnp.where(c == 0, theirs, mine)
    act = contract(seq_order(y), jnp.concatenate([zero, one], 0)).astype(BF16)

    of_seq = lax.broadcasted_iota(jnp.int32, (seqs, 1, tokens), 2) // length
    chosen = of_seq == lax.broadcasted_iota(jnp.int32, (seqs, 1, tokens), 0)
    masked = jnp.where(chosen, act[None], jnp.zeros((), BF16))
    partial_blocks = contract_last(masked, grads)
    pieces = partial_blocks.reshape(seqs, 8, 8, -1).swapaxes(0, 1)
    blocks = all_to_all(pieces, "seq").sum(0)
    squared = jnp.sum(blocks * blocks, axis=0)
    near, far = to_core_of_dp(squared)
    return (near + far) / (2 * seqs * 8 * length)


def solution(mesh):
    finer = Mesh(mesh.devices.reshape(2, 8, 8, 2, 2), ALL)
    in_specs = (P("dp", "seq", TENSOR), P("dp", "seq", TENSOR), P(TENSOR, "seq"), P(TENSOR, "seq"))
    out_specs = P(SEQ_TENSOR, None)

    return jax.shard_map(body, mesh=finer, in_specs=in_specs, out_specs=out_specs, check_vma=False)
```

```python
import jax
import jax.numpy as jnp
from jax import lax
from jax.experimental import pallas as pl
from jax.experimental.layout import Layout, with_layout_constraint
from jax.sharding import Mesh
from jax.experimental.pallas import tpu as pltpu
from jax.sharding import PartitionSpec as P


TENSOR = ("z", "x", "c")
SEQ_TENSOR = ("seq", "z", "x", "c")
ALL = ("dp", "seq", "z", "x", "c")
F32 = jnp.float32
BF16 = jnp.bfloat16


def exchange(v, axis):
    return lax.ppermute(v, axis, [(0, 1), (1, 0)])


def all_to_all(v, axis):
    return lax.all_to_all(v, axis, 0, 0, tiled=True)


def to_everyone(v, axis):
    return all_to_all(jnp.broadcast_to(v[None], (lax.axis_size(axis), *v.shape)), axis)


def contract_last(a, b):
    return lax.dot_general(
        a, b, (((a.ndim - 1,), (b.ndim - 1,)), ((), ())), preferred_element_type=F32
    )


def contract(a, b):
    return lax.dot_general(a, b, (((1,), (0,)), ((), ())), preferred_element_type=F32)


def seq_order(y):
    shape = (8, 8, 2, 4, 8)
    shard, row, core, slot, at = (lax.broadcasted_iota(jnp.int32, shape, k) for k in range(5))
    away = jnp.where(slot == 3, 4 * core, (slot + 1) * (2 * core - 1))
    picked = ((y + away - shard) % 8 == 0) & (row == at)
    return picked.astype(BF16).reshape(64, 64)


def grad_kernel(core, cols, own, other, out):
    lower = core[0] == 0
    rows = cols.shape[0] * cols.shape[2]
    first = jnp.where(lower, own[...], other[...])
    second = jnp.where(lower, other[...], own[...])
    out[...] = contract_last(cols[:, 0].reshape(rows, -1), first) + contract_last(
        cols[:, 1].reshape(rows, -1), second
    )


def early_kernel(one, two, three, here, there, out):
    width = here.shape[1]
    for k, block in enumerate((one, two, three)):
        found = contract_last(block[:, :width], here[...])
        found = found + contract_last(block[:, width:], there[...])
        out[:, k] = found.reshape(16, 8, -1).astype(BF16)


def last_kernel(core, own, far, here, there, filled, out):
    del filled
    width = here.shape[1]
    block = jnp.where(core[0] == 0, own[...], far[...])
    found = contract_last(block[:, :width], here[...])
    found = found + contract_last(block[:, width:], there[...])
    out[:, 0] = found.reshape(16, 8, -1).astype(BF16)


def projected_parts(c, block, steps, here, there):
    tokens, width = here.shape
    lanes = 256
    whole = pl.BlockSpec(block.shape, lambda n: (0, 0))
    rows = pl.BlockSpec((lanes, width), lambda n: (n, 0))
    shape = jax.ShapeDtypeStruct((16, 4, 8, tokens), BF16)
    filled = pl.pallas_call(
        early_kernel,
        grid=(tokens // lanes,),
        in_specs=[whole, whole, whole, rows, rows],
        out_specs=pl.BlockSpec((16, 4, 8, lanes), lambda n: (0, 0, 0, n)),
        out_shape=shape,
    )(*steps[:3], here, there)
    return pl.pallas_call(
        last_kernel,
        grid=(tokens // lanes,),
        in_specs=[
            pl.BlockSpec(memory_space=pltpu.SMEM),
            whole,
            whole,
            rows,
            rows,
            pl.BlockSpec(memory_space=pl.ANY),
        ],
        out_specs=pl.BlockSpec((16, 1, 8, lanes), lambda n: (0, 3, 0, n)),
        out_shape=shape,
        input_output_aliases={5: 0},
    )(c.reshape(1), block, steps[3], here, there, filled)


def ring_step(v, cores):
    n = lax.axis_size("seq")
    pairs = [(y * 2 + k, (y + 1 - 2 * k) % n * 2 + k) for y in range(n) for k in cores]
    return lax.ppermute(v, ("seq", "c"), pairs)


def to_core_of_dp(v):
    near = lax.ppermute(v, ("dp", "c"), [(d * 2 + c, c * 2 + d) for d in (0, 1) for c in (0, 1)])
    far = lax.ppermute(
        v, ("dp", "c"), [(d * 2 + c, (1 - c) * 2 + d) for d in (0, 1) for c in (0, 1)]
    )
    return near, far


def body(activations, gradients, basis_in, basis_out):
    d = lax.axis_index("dp")
    c = lax.axis_index("c")
    y = lax.axis_index("seq")
    seqs, length, width = activations.shape
    tokens = seqs * length
    x_own = activations.reshape(tokens, width)
    g_own = gradients.reshape(tokens, -1)

    x_far = exchange(x_own, "dp")

    halves = basis_out.T.reshape(1, 2, -1, basis_out.shape[0])
    spread = jnp.broadcast_to(halves, (8, *halves.shape[1:])).reshape(16, -1, basis_out.shape[0])
    out_cols = all_to_all(spread, ("seq", "c"))
    out_cols = out_cols.reshape(8, 2, -1, basis_out.shape[0])

    shard = with_layout_constraint(basis_in.T, Layout(major_to_minor=(0, 1)))
    half = shard.reshape(16, 2, 8, width)
    half = lax.dynamic_index_in_dim(half, d, 1, keepdims=False).reshape(128, width)
    partner = exchange(half, "c")
    g_other = exchange(g_own, "c")
    block = jnp.concatenate([half, partner], 1)
    step1 = ring_step(block, (0, 1))
    step2 = ring_step(step1, (0, 1))
    step3 = ring_step(step2, (0, 1))
    step4 = ring_step(step3, (1,))

    grad_partial = pl.pallas_call(
        grad_kernel,
        in_specs=[pl.BlockSpec(memory_space=pltpu.SMEM)]
        + [pl.BlockSpec(memory_space=pltpu.VMEM)] * 3,
        out_specs=pl.BlockSpec(memory_space=pltpu.VMEM),
        out_shape=jax.ShapeDtypeStruct((8 * out_cols.shape[2], tokens), F32),
    )(c.reshape(1), out_cols, g_own, g_other)
    grad_parts = all_to_all(grad_partial.reshape(16, -1, tokens), ("z", "x"))
    grad_own = grad_parts.sum(0).astype(BF16)
    grad_half = to_everyone(grad_own, ("z", "x")).reshape(8, -1, tokens)
    near, far = to_core_of_dp(grad_half)
    grads = jnp.where(d == 0, jnp.stack([near, far], 1), jnp.stack([far, near], 1))
    grads = grads.reshape(-1, tokens)

    x_rows = jnp.where(
        d == 0, jnp.concatenate([x_own, x_far], 0), jnp.concatenate([x_far, x_own], 0)
    )
    x_other = exchange(x_rows, "c")
    parts = projected_parts(c, block, (step1, step2, step3, step4), x_rows, x_other)
    arrived = all_to_all(parts, ("z", "x"))
    act = arrived.astype(F32).sum(0).astype(BF16).reshape(32, -1)

    left, right = act[:, :tokens], act[:, tokens:]
    mine = jnp.where(c == 0, left, right)
    theirs = exchange(jnp.where(c == 0, right, left), "c")
    zero = jnp.where(c == 0, mine, theirs)
    one = jnp.where(c == 0, theirs, mine)
    act = contract(seq_order(y), jnp.concatenate([zero, one], 0)).astype(BF16)

    of_seq = lax.broadcasted_iota(jnp.int32, (seqs, 1, tokens), 2) // length
    chosen = of_seq == lax.broadcasted_iota(jnp.int32, (seqs, 1, tokens), 0)
    masked = jnp.where(chosen, act[None], jnp.zeros((), BF16))
    partial_blocks = contract_last(masked, grads)
    pieces = partial_blocks.astype(BF16).reshape(seqs, 8, 8, -1).swapaxes(0, 1)
    blocks = all_to_all(pieces, "seq").astype(F32).sum(0)
    squared = jnp.sum(blocks * blocks, axis=0)
    near, far = to_core_of_dp(squared)
    return (near + far) / (2 * seqs * 8 * length)


def solution(mesh):
    finer = Mesh(mesh.devices.reshape(2, 8, 8, 2, 2), ALL)
    in_specs = (P("dp", "seq", TENSOR), P("dp", "seq", TENSOR), P(TENSOR, "seq"), P(TENSOR, "seq"))
    out_specs = P(SEQ_TENSOR, None)

    return jax.shard_map(body, mesh=finer, in_specs=in_specs, out_specs=out_specs, check_vma=False)
```

```python
import jax
import jax.numpy as jnp
from jax import lax
from jax.experimental import pallas as pl
from jax.experimental.layout import Layout, with_layout_constraint
from jax.sharding import Mesh
from jax.experimental.pallas import tpu as pltpu
from jax.sharding import PartitionSpec as P


TENSOR = ("z", "x", "c")
SEQ_TENSOR = ("seq", "z", "x", "c")
ALL = ("dp", "seq", "z", "x", "c")
F32 = jnp.float32
BF16 = jnp.bfloat16


def exchange(v, axis):
    return lax.ppermute(v, axis, [(0, 1), (1, 0)])


def all_to_all(v, axis):
    return lax.all_to_all(v, axis, 0, 0, tiled=True)


def contract_last(a, b):
    return lax.dot_general(
        a, b, (((a.ndim - 1,), (b.ndim - 1,)), ((), ())), preferred_element_type=F32
    )


def contract(a, b):
    return lax.dot_general(a, b, (((1,), (0,)), ((), ())), preferred_element_type=F32)


def seq_order(y):
    shape = (8, 8, 2, 4, 8)
    shard, row, core, slot, at = (lax.broadcasted_iota(jnp.int32, shape, k) for k in range(5))
    away = jnp.where(slot == 3, 4 * core, (slot + 1) * (2 * core - 1))
    picked = ((y + away - shard) % 8 == 0) & (row == at)
    return picked.astype(BF16).reshape(64, 64)


def grad_kernel(core, cols, own, other, out):
    lower = core[0] == 0
    rows = cols.shape[0] * cols.shape[2]
    first = jnp.where(lower, own[...], other[...])
    second = jnp.where(lower, other[...], own[...])
    found = contract_last(cols[:, 0].reshape(rows, -1), first)
    found = found + contract_last(cols[:, 1].reshape(rows, -1), second)
    out[...] = found.astype(BF16)


def product(block, here, there):
    width = here.shape[1]
    found = contract_last(here[...], block[:, :width])
    found = found + contract_last(there[...], block[:, width:])
    return found.T.reshape(16, 8, -1).astype(BF16)


def early_kernel(one, two, three, here, there, out):
    for k, block in enumerate((one, two, three)):
        out[:, k] = product(block[...], here, there)


def last_kernel(core, own, far, here, there, filled, out):
    del filled
    out[:, 0] = product(jnp.where(core[0] == 0, own[...], far[...]), here, there)


def projected_parts(c, block, steps, here, there):
    tokens, width = here.shape
    lanes = 256
    whole = pl.BlockSpec(block.shape, lambda n: (0, 0))
    rows = pl.BlockSpec((lanes, width), lambda n: (n, 0))
    shape = jax.ShapeDtypeStruct((16, 4, 8, tokens), BF16)
    filled = pl.pallas_call(
        early_kernel,
        grid=(tokens // lanes,),
        in_specs=[whole, whole, whole, rows, rows],
        out_specs=pl.BlockSpec((16, 4, 8, lanes), lambda n: (0, 0, 0, n)),
        out_shape=shape,
    )(*steps[:3], here, there)
    return pl.pallas_call(
        last_kernel,
        grid=(tokens // lanes,),
        in_specs=[
            pl.BlockSpec(memory_space=pltpu.SMEM),
            whole,
            whole,
            rows,
            rows,
            pl.BlockSpec(memory_space=pl.ANY),
        ],
        out_specs=pl.BlockSpec((16, 1, 8, lanes), lambda n: (0, 3, 0, n)),
        out_shape=shape,
        input_output_aliases={5: 0},
    )(c.reshape(1), block, steps[3], here, there, filled)


def ring_step(v, cores):
    n = lax.axis_size("seq")
    pairs = [(y * 2 + k, (y + 1 - 2 * k) % n * 2 + k) for y in range(n) for k in cores]
    return lax.ppermute(v, ("seq", "c"), pairs)


def doubled(v, axis, bit):
    n = lax.axis_size(axis)
    other = lax.ppermute(v, axis, [(i, i ^ bit) for i in range(n)])
    low = lax.axis_index(axis) & bit == 0
    both = jnp.where(low, jnp.stack([v, other], 1), jnp.stack([other, v], 1))
    return both.reshape(-1, *v.shape[1:])


def to_core_of_dp(v):
    near = lax.ppermute(v, ("dp", "c"), [(d * 2 + c, c * 2 + d) for d in (0, 1) for c in (0, 1)])
    far = lax.ppermute(
        v, ("dp", "c"), [(d * 2 + c, (1 - c) * 2 + d) for d in (0, 1) for c in (0, 1)]
    )
    return near, far


def body(activations, gradients, basis_in, basis_out):
    d = lax.axis_index("dp")
    c = lax.axis_index("c")
    y = lax.axis_index("seq")
    seqs, length, width = activations.shape
    tokens = seqs * length
    x_own = activations.reshape(tokens, width)
    g_own = gradients.reshape(tokens, -1)

    x_far = exchange(x_own, "dp")

    halves = basis_out.T.reshape(1, 2, -1, basis_out.shape[0])
    spread = jnp.broadcast_to(halves, (8, *halves.shape[1:])).reshape(16, -1, basis_out.shape[0])
    out_cols = all_to_all(spread, ("seq", "c"))
    out_cols = out_cols.reshape(8, 2, -1, basis_out.shape[0])

    shard = with_layout_constraint(basis_in.T, Layout(major_to_minor=(0, 1)))
    half = shard.reshape(16, 2, 8, width)
    half = lax.dynamic_index_in_dim(half, d, 1, keepdims=False).reshape(128, width)
    partner = exchange(half, "c")
    g_other = exchange(g_own, "c")
    block = jnp.concatenate([half, partner], 1)
    step1 = ring_step(block, (0, 1))
    step2 = ring_step(step1, (0, 1))
    step3 = ring_step(step2, (0, 1))
    step4 = ring_step(step3, (1,))

    grad_partial = pl.pallas_call(
        grad_kernel,
        in_specs=[pl.BlockSpec(memory_space=pltpu.SMEM)]
        + [pl.BlockSpec(memory_space=pltpu.VMEM)] * 3,
        out_specs=pl.BlockSpec(memory_space=pltpu.VMEM),
        out_shape=jax.ShapeDtypeStruct((8 * out_cols.shape[2], tokens), BF16),
    )(c.reshape(1), out_cols, g_own, g_other)
    grad_parts = all_to_all(grad_partial.reshape(16, -1, tokens), ("z", "x"))
    grad_half = grad_parts.astype(F32).sum(0).astype(BF16)[None]
    for axis, bit in (("z", 4), ("z", 2), ("z", 1), ("x", 1)):
        grad_half = doubled(grad_half, axis, bit)
    grad_half = grad_half.reshape(8, -1, tokens)
    near, far = to_core_of_dp(grad_half)
    grads = jnp.where(d == 0, jnp.stack([near, far], 1), jnp.stack([far, near], 1))
    grads = grads.reshape(-1, tokens)

    x_rows = jnp.where(
        d == 0, jnp.concatenate([x_own, x_far], 0), jnp.concatenate([x_far, x_own], 0)
    )
    x_other = exchange(x_rows, "c")
    parts = projected_parts(c, block, (step1, step2, step3, step4), x_rows, x_other)
    arrived = all_to_all(parts, ("z", "x"))
    act = arrived.astype(F32).sum(0).astype(BF16).reshape(32, -1)

    left, right = act[:, :tokens], act[:, tokens:]
    mine = jnp.where(c == 0, left, right)
    theirs = exchange(jnp.where(c == 0, right, left), "c")
    zero = jnp.where(c == 0, mine, theirs)
    one = jnp.where(c == 0, theirs, mine)
    act = contract(seq_order(y), jnp.concatenate([zero, one], 0)).astype(BF16)

    of_seq = lax.broadcasted_iota(jnp.int32, (seqs, 1, tokens), 2) // length
    chosen = of_seq == lax.broadcasted_iota(jnp.int32, (seqs, 1, tokens), 0)
    masked = jnp.where(chosen, act[None], jnp.zeros((), BF16))
    partial_blocks = contract_last(masked, grads)
    pieces = partial_blocks.astype(BF16).reshape(seqs, 8, 8, -1).swapaxes(0, 1)
    blocks = all_to_all(pieces, "seq").astype(F32).sum(0)
    squared = jnp.sum(blocks * blocks, axis=0)
    near, far = to_core_of_dp(squared)
    return (near + far) / (2 * seqs * 8 * length)


def solution(mesh):
    finer = Mesh(mesh.devices.reshape(2, 8, 8, 2, 2), ALL)
    in_specs = (P("dp", "seq", TENSOR), P("dp", "seq", TENSOR), P(TENSOR, "seq"), P(TENSOR, "seq"))
    out_specs = P(SEQ_TENSOR, None)

    return jax.shard_map(body, mesh=finer, in_specs=in_specs, out_specs=out_specs, check_vma=False)
```

```python
import jax
import jax.numpy as jnp
from jax import lax
from jax.experimental import pallas as pl
from jax.experimental.layout import Layout, with_layout_constraint
from jax.sharding import Mesh
from jax.experimental.pallas import tpu as pltpu
from jax.sharding import PartitionSpec as P


TENSOR = ("z", "x", "c")
SEQ_TENSOR = ("seq", "z", "x", "c")
ALL = ("dp", "seq", "z", "x", "c")
F32 = jnp.float32
BF16 = jnp.bfloat16


def exchange(v, axis):
    return lax.ppermute(v, axis, [(0, 1), (1, 0)])


def all_to_all(v, axis):
    return lax.all_to_all(v, axis, 0, 0, tiled=True)


def to_everyone(v, axis):
    return all_to_all(jnp.broadcast_to(v[None], (lax.axis_size(axis), *v.shape)), axis)


def contract_last(a, b):
    return lax.dot_general(
        a, b, (((a.ndim - 1,), (b.ndim - 1,)), ((), ())), preferred_element_type=F32
    )


def grad_kernel(core, cols, own, other, out):
    lower = core[0] == 0
    rows = cols.shape[0] * cols.shape[2]
    width = own.shape[1]
    parts = own.shape[0] // other.shape[0]
    start = other.shape[1] - parts * width
    theirs = [other[:, start + k * width : start + (k + 1) * width] for k in range(parts)]
    theirs = jnp.concatenate(theirs, 0)
    first = jnp.where(lower, own[...], theirs)
    second = jnp.where(lower, theirs, own[...])
    out[...] = contract_last(cols[:, 0].reshape(rows, -1), first) + contract_last(
        cols[:, 1].reshape(rows, -1), second
    )


def body(activations, gradients, basis_in, basis_out):
    c = lax.axis_index("c")
    seqs, length, width = activations.shape
    tokens = seqs * length
    x_own = activations.reshape(tokens, width)
    g_own = gradients.reshape(tokens, -1)

    shard = with_layout_constraint(basis_in.T, Layout(major_to_minor=(0, 1)))
    shard = shard.reshape(16, 2, 8, width)
    half = lax.dynamic_index_in_dim(shard, c, 1, keepdims=False).reshape(128, width)
    other = lax.dynamic_index_in_dim(shard, 1 - c, 1, keepdims=False).reshape(128, width)
    folded = [g_own[k * 128 : (k + 1) * 128] for k in range(tokens // 128)]
    partner = exchange(jnp.concatenate([other, *folded], 1), "c")
    block = jnp.concatenate([half, partner[:, :width]], 1)
    columns = lax.all_gather(block, "seq", axis=0, tiled=True)
    x_other = exchange(x_own, "c")

    halves = basis_out.T.reshape(1, 2, -1, basis_out.shape[0])
    spread = jnp.broadcast_to(halves, (8, *halves.shape[1:])).reshape(16, -1, basis_out.shape[0])
    out_cols = all_to_all(spread, ("seq", "c"))
    out_cols = out_cols.reshape(8, 2, -1, basis_out.shape[0])

    grad_partial = pl.pallas_call(
        grad_kernel,
        in_specs=[pl.BlockSpec(memory_space=pltpu.SMEM)]
        + [pl.BlockSpec(memory_space=pltpu.VMEM)] * 3,
        out_specs=pl.BlockSpec(memory_space=pltpu.VMEM),
        out_shape=jax.ShapeDtypeStruct((8 * out_cols.shape[2], tokens), F32),
    )(c.reshape(1), out_cols, g_own, partner)
    grad_parts = all_to_all(grad_partial.reshape(16, -1, tokens), ("z", "x"))
    grad_own = grad_parts.sum(0).astype(BF16)
    grad_half = to_everyone(grad_own, ("z", "x")).reshape(8, -1, tokens)
    grad_rest = exchange(grad_half, "c")
    grads = jnp.where(
        c == 0, jnp.stack([grad_half, grad_rest], 1), jnp.stack([grad_rest, grad_half], 1)
    ).reshape(-1, tokens)

    x_rows = lax.optimization_barrier(jnp.concatenate([x_own, x_other], 1))
    parts = contract_last(columns, x_rows).astype(BF16)
    parts = parts.reshape(8, 16, 8, tokens).swapaxes(0, 1)
    arrived = all_to_all(parts, ("z", "x"))
    act = arrived.astype(F32).sum(0).astype(BF16).reshape(64, tokens)

    of_seq = lax.broadcasted_iota(jnp.int32, (seqs, 1, tokens), 2) // length
    chosen = of_seq == lax.broadcasted_iota(jnp.int32, (seqs, 1, tokens), 0)
    masked = jnp.where(chosen, act[None], jnp.zeros((), BF16))
    partial_blocks = contract_last(masked, grads)
    pieces = partial_blocks.astype(BF16).reshape(seqs, 8, 8, -1).swapaxes(0, 1)
    blocks = all_to_all(pieces, "seq").astype(F32).sum(0)
    squared = jnp.sum(blocks * blocks, axis=0)
    far = exchange(squared, "dp")
    return (squared + far) / (2 * seqs * 8 * length)


def solution(mesh):
    finer = Mesh(mesh.devices.reshape(2, 8, 8, 2, 2), ALL)
    in_specs = (P("dp", "seq", TENSOR), P("dp", "seq", TENSOR), P(TENSOR, "seq"), P(TENSOR, "seq"))
    out_specs = P(SEQ_TENSOR, None)

    return jax.shard_map(body, mesh=finer, in_specs=in_specs, out_specs=out_specs, check_vma=False)
```

```python
import jax
import jax.numpy as jnp
from jax import lax
from jax.experimental import pallas as pl
from jax.experimental.layout import Layout, with_layout_constraint
from jax.sharding import Mesh
from jax.experimental.pallas import tpu as pltpu
from jax.sharding import PartitionSpec as P


TENSOR = ("z", "x", "c")
SEQ_TENSOR = ("seq", "z", "x", "c")
ALL = ("dp", "seq", "z", "x", "c")
F32 = jnp.float32
BF16 = jnp.bfloat16


def exchange(v, axis):
    return lax.ppermute(v, axis, [(0, 1), (1, 0)])


def all_to_all(v, axis):
    return lax.all_to_all(v, axis, 0, 0, tiled=True)


def to_everyone(v, axis):
    return all_to_all(jnp.broadcast_to(v[None], (lax.axis_size(axis), *v.shape)), axis)


def contract_last(a, b):
    return lax.dot_general(
        a, b, (((a.ndim - 1,), (b.ndim - 1,)), ((), ())), preferred_element_type=F32
    )


def grad_kernel(cols, own, beside, pair, out):
    rows = cols.shape[0] * cols.shape[2]
    found = jnp.zeros(out.shape, F32)
    for k, features in enumerate((own[...], pair[0], beside[...], pair[1])):
        columns = cols[:, k].astype(F32).reshape(rows, -1).astype(BF16)
        found = found + contract_last(columns, features)
    out[...] = found


def body(activations, gradients, basis_in, basis_out):
    x = lax.axis_index("x")
    c = lax.axis_index("c")
    seqs, length, width = activations.shape
    tokens = seqs * length
    narrow = basis_out.shape[0]
    x_own = activations.reshape(tokens, width)
    g_own = gradients.reshape(tokens, narrow)

    shard = with_layout_constraint(basis_in.T, Layout(major_to_minor=(0, 1)))
    shard = shard.reshape(8, 4, 8, width).swapaxes(0, 1).reshape(4, 64, width)
    small = jnp.pad(basis_out.T.reshape(4, 24, narrow), ((0, 0), (0, 0), (0, width - narrow)))
    quarter = all_to_all(jnp.concatenate([shard, small], 1), ("x", "c"))
    near = [
        lax.dynamic_index_in_dim(quarter, (x * 2 + c) ^ k, 0, keepdims=False) for k in range(4)
    ]
    block = jnp.concatenate([piece[:64] for piece in near], 1)
    columns = lax.all_gather(block, "seq", axis=0, tiled=True)
    small = jnp.stack([piece[64:, :narrow] for piece in near])

    g_beside = exchange(g_own, "x")
    g_pair = exchange(jnp.stack([g_own, g_beside]), "c")
    x_beside = exchange(x_own, "x")
    x_pair = exchange(jnp.stack([x_own, x_beside]), "c")

    out_cols = to_everyone(small, "seq")
    grad_partial = pl.pallas_call(
        grad_kernel,
        in_specs=[pl.BlockSpec(memory_space=pltpu.VMEM)] * 4,
        out_specs=pl.BlockSpec(memory_space=pltpu.VMEM),
        out_shape=jax.ShapeDtypeStruct((8 * 24, tokens), F32),
    )(out_cols, g_own, g_beside, g_pair)
    grad_parts = all_to_all(grad_partial.reshape(8, 24, tokens), "z")
    grad_own = grad_parts.sum(0).astype(BF16)
    grad_quarter = to_everyone(grad_own, "z")
    rest = exchange(grad_quarter, "x")
    grad_half = jnp.where(x == 0, jnp.stack([grad_quarter, rest]), jnp.stack([rest, grad_quarter]))
    rest = exchange(grad_half, "c")
    grads = jnp.where(c == 0, jnp.stack([grad_half, rest]), jnp.stack([rest, grad_half]))
    grads = grads.transpose(2, 1, 0, 3, 4).reshape(-1, tokens)

    x_rows = jnp.concatenate([x_own, x_pair[0], x_beside, x_pair[1]], 1)
    x_rows = lax.optimization_barrier(x_rows)
    parts = contract_last(columns, x_rows).astype(BF16)
    parts = parts.reshape(8, 8, 8, tokens).swapaxes(0, 1)
    arrived = all_to_all(parts, "z")
    act = arrived.astype(F32).sum(0).astype(BF16).reshape(64, tokens)

    of_seq = lax.broadcasted_iota(jnp.int32, (seqs, 1, tokens), 2) // length
    chosen = of_seq == lax.broadcasted_iota(jnp.int32, (seqs, 1, tokens), 0)
    masked = jnp.where(chosen, act[None], jnp.zeros((), BF16))
    partial_blocks = contract_last(masked, grads)
    pieces = partial_blocks.astype(BF16).reshape(seqs, 8, 8, -1).swapaxes(0, 1)
    blocks = all_to_all(pieces, "seq").astype(F32).sum(0)
    squared = jnp.sum(blocks * blocks, axis=0)
    far = exchange(squared, "dp")
    return (squared + far) / (2 * seqs * 8 * length)


def solution(mesh):
    finer = Mesh(mesh.devices.reshape(2, 8, 8, 2, 2), ALL)
    in_specs = (P("dp", "seq", TENSOR), P("dp", "seq", TENSOR), P(TENSOR, "seq"), P(TENSOR, "seq"))
    out_specs = P(SEQ_TENSOR, None)

    return jax.shard_map(body, mesh=finer, in_specs=in_specs, out_specs=out_specs, check_vma=False)
```

```python
import jax
import jax.numpy as jnp
from jax import lax
from jax.experimental import pallas as pl
from jax.experimental.layout import Layout, with_layout_constraint
from jax.sharding import Mesh
from jax.experimental.pallas import tpu as pltpu
from jax.sharding import PartitionSpec as P


TENSOR = ("z", "x", "c")
SEQ_TENSOR = ("seq", "z", "x", "c")
ALL = ("dp", "seq", "z", "x", "c")
F32 = jnp.float32
BF16 = jnp.bfloat16


def exchange(v, axis):
    return lax.ppermute(v, axis, [(0, 1), (1, 0)])


def all_to_all(v, axis):
    return lax.all_to_all(v, axis, 0, 0, tiled=True)


def to_everyone(v, axis):
    return all_to_all(jnp.broadcast_to(v[None], (lax.axis_size(axis), *v.shape)), axis)


def contract_last(a, b):
    return lax.dot_general(
        a, b, (((a.ndim - 1,), (b.ndim - 1,)), ((), ())), preferred_element_type=F32
    )


def to_owner(v, across):
    pairs = []
    for d in range(2):
        for pair in range(4):
            for a in range(2):
                for b in range(2):
                    source = (d * 8 + pair * 2 + b) * 2 + a
                    pairs.append((source, ((d ^ across) * 8 + pair * 2 + a) * 2 + b))
    return lax.ppermute(v, ("dp", "seq", "x"), pairs)


def grad_kernel(place, cols, own, beside, pair, out):
    rows = cols.shape[0] * cols.shape[2]
    found = jnp.zeros(out.shape, F32)
    for k, features in enumerate((own[...], pair[0], beside[...], pair[1])):
        columns = cols[:, pl.ds(place[k], 1)].astype(F32).reshape(rows, -1).astype(BF16)
        found = found + contract_last(columns, features)
    out[...] = found


def body(activations, gradients, basis_in, basis_out):
    d = lax.axis_index("dp")
    x = lax.axis_index("x")
    c = lax.axis_index("c")
    seqs, length, width = activations.shape
    tokens = seqs * length
    x_own = activations.reshape(tokens, width)
    narrow = basis_out.shape[0]
    g_own = gradients.reshape(tokens, narrow)

    shard = with_layout_constraint(basis_in.T, Layout(major_to_minor=(0, 1)))
    shard = shard.reshape(8, 4, 8, width)
    half = lax.dynamic_index_in_dim(shard, d * 2 + c, 1, keepdims=False).reshape(64, width)
    other = lax.dynamic_index_in_dim(shard, d * 2 + 1 - c, 1, keepdims=False).reshape(64, width)
    partner = exchange(other, "c")
    block = jnp.concatenate([half, partner], 1)
    columns = lax.all_gather(block, "seq", axis=0, tiled=True)
    x_far = exchange(x_own, "dp")

    spread = jnp.broadcast_to(basis_out.T.reshape(1, 4, 24, narrow), (8, 4, 24, narrow))
    out_cols = all_to_all(spread.reshape(32, 24, narrow), ("seq", "x", "c"))
    out_cols = out_cols.reshape(8, 4, 24, narrow)
    g_beside = exchange(g_own, "x")
    g_pair = exchange(jnp.stack([g_own, g_beside]), "c")

    place = (x * 2 + c) ^ jnp.arange(4, dtype=jnp.int32)
    grad_partial = pl.pallas_call(
        grad_kernel,
        in_specs=[pl.BlockSpec(memory_space=pltpu.SMEM)]
        + [pl.BlockSpec(memory_space=pltpu.VMEM)] * 4,
        out_specs=pl.BlockSpec(memory_space=pltpu.VMEM),
        out_shape=jax.ShapeDtypeStruct((8 * 24, tokens), F32),
    )(place, out_cols, g_own, g_beside, g_pair)
    grad_parts = all_to_all(grad_partial.reshape(8, 24, tokens), "z")
    grad_parts, x_far = lax.optimization_barrier((grad_parts, x_far))
    x_rows = jnp.concatenate([x_own, x_far], 0)
    x_other = exchange(x_rows, "c")
    grad_own = grad_parts.sum(0).astype(BF16)
    grad_quarter = to_everyone(grad_own, "z")
    rest = exchange(grad_quarter, "x")
    grad_half = jnp.where(x == 0, jnp.stack([grad_quarter, rest]), jnp.stack([rest, grad_quarter]))
    rest = exchange(grad_half, "c")
    grads = jnp.where(c == 0, jnp.stack([grad_half, rest]), jnp.stack([rest, grad_half]))
    grads = grads.transpose(2, 1, 0, 3, 4).reshape(-1, tokens)

    x_rows = lax.optimization_barrier(jnp.concatenate([x_rows, x_other], 1))
    parts = contract_last(columns, x_rows).astype(BF16)
    parts = parts.reshape(4, 2, 8, 8, -1).transpose(2, 1, 0, 3, 4)
    arrived = all_to_all(parts.reshape(16, 4, 8, -1), ("z", "x"))
    act = arrived.astype(F32).sum(0).astype(BF16).reshape(32, -1)

    mine = act[:, :tokens]
    theirs = exchange(act[:, tokens:], "dp")
    act = jnp.where(d == 0, jnp.stack([mine, theirs]), jnp.stack([theirs, mine]))
    act = act.reshape(2, 4, 8, tokens).swapaxes(0, 1).reshape(64, tokens)

    of_seq = lax.broadcasted_iota(jnp.int32, (seqs, 1, tokens), 2) // length
    chosen = of_seq == lax.broadcasted_iota(jnp.int32, (seqs, 1, tokens), 0)
    masked = jnp.where(chosen, act[None], jnp.zeros((), BF16))
    partial_blocks = contract_last(masked, grads)
    pieces = partial_blocks.astype(BF16).reshape(seqs, 8, 8, -1).swapaxes(0, 1)
    blocks = all_to_all(pieces, "seq").astype(F32).sum(0)
    squared = jnp.sum(blocks * blocks, axis=0)
    near, far = (to_owner(squared, across) for across in (0, 1))
    return (near + far) / (2 * seqs * 8 * length)


def solution(mesh):
    finer = Mesh(mesh.devices.reshape(2, 8, 8, 2, 2), ALL)
    in_specs = (P("dp", "seq", TENSOR), P("dp", "seq", TENSOR), P(TENSOR, "seq"), P(TENSOR, "seq"))
    out_specs = P(SEQ_TENSOR, None)

    return jax.shard_map(body, mesh=finer, in_specs=in_specs, out_specs=out_specs, check_vma=False)
```

```python
import jax
import jax.numpy as jnp
from jax import lax
from jax.experimental import pallas as pl
from jax.experimental.layout import Layout, with_layout_constraint
from jax.sharding import Mesh
from jax.experimental.pallas import tpu as pltpu
from jax.sharding import PartitionSpec as P


TENSOR = ("z", "x", "c")
SEQ_TENSOR = ("seq", "z", "x", "c")
ALL = ("dp", "seq", "z", "x", "c")
F32 = jnp.float32
BF16 = jnp.bfloat16


def exchange(v, axis):
    return lax.ppermute(v, axis, [(0, 1), (1, 0)])


def all_to_all(v, axis):
    return lax.all_to_all(v, axis, 0, 0, tiled=True)


def to_everyone(v, axis):
    return all_to_all(jnp.broadcast_to(v[None], (lax.axis_size(axis), *v.shape)), axis)


def contract_last(a, b):
    return lax.dot_general(
        a, b, (((a.ndim - 1,), (b.ndim - 1,)), ((), ())), preferred_element_type=F32
    )


def grad_kernel(place, cols, own, beside, pair, out):
    rows = cols.shape[0] * cols.shape[2]
    found = jnp.zeros(out.shape, F32)
    for k, features in enumerate((own[...], pair[0], beside[...], pair[1])):
        columns = cols[:, pl.ds(place[k], 1)].astype(F32).reshape(rows, -1).astype(BF16)
        found = found + contract_last(columns, features)
    out[...] = found


def body(activations, gradients, basis_in, basis_out):
    x = lax.axis_index("x")
    c = lax.axis_index("c")
    seqs, length, width = activations.shape
    tokens = seqs * length
    x_own = activations.reshape(tokens, width)
    narrow = basis_out.shape[0]
    g_own = gradients.reshape(tokens, narrow)

    shard = with_layout_constraint(basis_in.T, Layout(major_to_minor=(0, 1)))
    shard = shard.reshape(16, 2, 8, width)
    half = lax.dynamic_index_in_dim(shard, c, 1, keepdims=False).reshape(128, width)
    other = lax.dynamic_index_in_dim(shard, 1 - c, 1, keepdims=False).reshape(128, width)
    partner = exchange(other, "c")
    block = jnp.concatenate([half, partner], 1)
    columns = lax.all_gather(block, "seq", axis=0, tiled=True)
    x_other = exchange(x_own, "c")

    spread = jnp.broadcast_to(basis_out.T.reshape(1, 4, 24, narrow), (8, 4, 24, narrow))
    out_cols = all_to_all(spread.reshape(32, 24, narrow), ("seq", "x", "c"))
    out_cols = out_cols.reshape(8, 4, 24, narrow)
    g_beside = exchange(g_own, "x")
    g_pair = exchange(jnp.stack([g_own, g_beside]), "c")

    place = (x * 2 + c) ^ jnp.arange(4, dtype=jnp.int32)
    grad_partial = pl.pallas_call(
        grad_kernel,
        in_specs=[pl.BlockSpec(memory_space=pltpu.SMEM)]
        + [pl.BlockSpec(memory_space=pltpu.VMEM)] * 4,
        out_specs=pl.BlockSpec(memory_space=pltpu.VMEM),
        out_shape=jax.ShapeDtypeStruct((8 * 24, tokens), F32),
    )(place, out_cols, g_own, g_beside, g_pair)
    grad_parts = all_to_all(grad_partial.reshape(8, 24, tokens), "z")
    grad_own = grad_parts.sum(0).astype(BF16)
    grad_quarter = to_everyone(grad_own, "z")
    rest = exchange(grad_quarter, "x")
    grad_half = jnp.where(x == 0, jnp.stack([grad_quarter, rest]), jnp.stack([rest, grad_quarter]))
    rest = exchange(grad_half, "c")
    grads = jnp.where(c == 0, jnp.stack([grad_half, rest]), jnp.stack([rest, grad_half]))
    grads = grads.transpose(2, 1, 0, 3, 4).reshape(-1, tokens)

    x_rows = lax.optimization_barrier(jnp.concatenate([x_own, x_other], 1))
    parts = contract_last(columns, x_rows).astype(BF16)
    parts = parts.reshape(8, 8, 2, 8, tokens).transpose(2, 1, 0, 3, 4).reshape(16, 8, 8, tokens)
    arrived = all_to_all(parts, ("x", "z"))
    act = arrived.astype(F32).sum(0).astype(BF16).reshape(64, tokens)

    of_seq = lax.broadcasted_iota(jnp.int32, (seqs, 1, tokens), 2) // length
    chosen = of_seq == lax.broadcasted_iota(jnp.int32, (seqs, 1, tokens), 0)
    masked = jnp.where(chosen, act[None], jnp.zeros((), BF16))
    partial_blocks = contract_last(masked, grads)
    pieces = partial_blocks.astype(BF16).reshape(seqs, 8, 8, -1).swapaxes(0, 1)
    blocks = all_to_all(pieces, "seq").astype(F32).sum(0)
    squared = jnp.sum(blocks * blocks, axis=0)
    far = exchange(squared, "dp")
    return (squared + far) / (2 * seqs * 8 * length)


def solution(mesh):
    finer = Mesh(mesh.devices.reshape(2, 8, 8, 2, 2), ALL)
    in_specs = (P("dp", "seq", TENSOR), P("dp", "seq", TENSOR), P(TENSOR, "seq"), P(TENSOR, "seq"))
    out_specs = P(SEQ_TENSOR, None)

    return jax.shard_map(body, mesh=finer, in_specs=in_specs, out_specs=out_specs, check_vma=False)
```

```python
import jax
import jax.numpy as jnp
from jax import lax
from jax.experimental import pallas as pl
from jax.experimental.layout import Layout, with_layout_constraint
from jax.sharding import Mesh
from jax.experimental.pallas import tpu as pltpu
from jax.sharding import PartitionSpec as P


TENSOR = ("z", "x", "c")
SEQ_TENSOR = ("seq", "z", "x", "c")
ALL = ("dp", "seq", "z", "x", "c")
F32 = jnp.float32
BF16 = jnp.bfloat16


def exchange(v, axis):
    return lax.ppermute(v, axis, [(0, 1), (1, 0)])


def all_to_all(v, axis):
    return lax.all_to_all(v, axis, 0, 0, tiled=True)


def to_everyone(v, axis):
    return all_to_all(jnp.broadcast_to(v[None], (lax.axis_size(axis), *v.shape)), axis)


def contract_last(a, b):
    return lax.dot_general(
        a, b, (((a.ndim - 1,), (b.ndim - 1,)), ((), ())), preferred_element_type=F32
    )


def grad_kernel(place, cols, own, beside, pair, out):
    rows = cols.shape[1] * cols.shape[2]
    found = jnp.zeros(out.shape, F32)
    for k, features in enumerate((own[...], pair[0], beside[...], pair[1])):
        columns = cols[pl.ds(place[k], 1)].astype(F32).reshape(rows, -1).astype(BF16)
        found = found + contract_last(columns, features)
    out[...] = found


def body(activations, gradients, basis_in, basis_out):
    x = lax.axis_index("x")
    c = lax.axis_index("c")
    seqs, length, width = activations.shape
    tokens = seqs * length
    x_own = activations.reshape(tokens, width)
    narrow = basis_out.shape[0]
    g_own = gradients.reshape(tokens, narrow)

    shard = with_layout_constraint(basis_in.T, Layout(major_to_minor=(0, 1)))
    shard = shard.reshape(16, 2, 8, width)
    half = lax.dynamic_index_in_dim(shard, c, 1, keepdims=False).reshape(128, width)
    other = lax.dynamic_index_in_dim(shard, 1 - c, 1, keepdims=False).reshape(128, width)
    partner = exchange(other, "c")
    block = jnp.concatenate([half, partner], 1)
    columns = lax.all_gather(block, "seq", axis=0, tiled=True)
    x_other = exchange(x_own, "c")

    spread = jnp.broadcast_to(basis_out.T.reshape(4, 1, 24, narrow), (4, 8, 24, narrow))
    out_cols = all_to_all(spread.reshape(32, 24, narrow), ("x", "c", "seq"))
    out_cols = out_cols.reshape(4, 8, 24, narrow)
    g_beside = exchange(g_own, "x")
    g_pair = exchange(jnp.stack([g_own, g_beside]), "c")

    place = (x * 2 + c) ^ jnp.arange(4, dtype=jnp.int32)
    grad_partial = pl.pallas_call(
        grad_kernel,
        in_specs=[pl.BlockSpec(memory_space=pltpu.SMEM)]
        + [pl.BlockSpec(memory_space=pltpu.VMEM)] * 4,
        out_specs=pl.BlockSpec(memory_space=pltpu.VMEM),
        out_shape=jax.ShapeDtypeStruct((8 * 24, tokens), F32),
    )(place, out_cols, g_own, g_beside, g_pair)
    grad_parts = all_to_all(grad_partial.reshape(8, 24, tokens), "z")
    grad_own = grad_parts.sum(0).astype(BF16)
    grad_quarter = to_everyone(grad_own, "z")
    rest = exchange(grad_quarter, "x")
    grad_half = jnp.where(x == 0, jnp.stack([grad_quarter, rest]), jnp.stack([rest, grad_quarter]))
    rest = exchange(grad_half, "c")
    grads = jnp.where(c == 0, jnp.stack([grad_half, rest]), jnp.stack([rest, grad_half]))
    grads = grads.transpose(2, 1, 0, 3, 4).reshape(-1, tokens)

    x_rows = lax.optimization_barrier(jnp.concatenate([x_own, x_other], 1))
    parts = contract_last(columns, x_rows).astype(BF16)
    parts = parts.reshape(8, 8, 2, 8, tokens).transpose(2, 1, 0, 3, 4).reshape(16, 8, 8, tokens)
    arrived = all_to_all(parts, ("x", "z"))
    act = arrived.astype(F32).sum(0).astype(BF16).reshape(64, tokens)

    of_seq = lax.broadcasted_iota(jnp.int32, (seqs, 1, tokens), 2) // length
    chosen = of_seq == lax.broadcasted_iota(jnp.int32, (seqs, 1, tokens), 0)
    masked = jnp.where(chosen, act[None], jnp.zeros((), BF16))
    partial_blocks = contract_last(masked, grads)
    pieces = partial_blocks.astype(BF16).reshape(seqs, 8, 8, -1).swapaxes(0, 1)
    blocks = all_to_all(pieces, "seq").astype(F32).sum(0)
    squared = jnp.sum(blocks * blocks, axis=0)
    far = exchange(squared, "dp")
    return (squared + far) / (2 * seqs * 8 * length)


def solution(mesh):
    finer = Mesh(mesh.devices.reshape(2, 8, 8, 2, 2), ALL)
    in_specs = (P("dp", "seq", TENSOR), P("dp", "seq", TENSOR), P(TENSOR, "seq"), P(TENSOR, "seq"))
    out_specs = P(SEQ_TENSOR, None)

    return jax.shard_map(body, mesh=finer, in_specs=in_specs, out_specs=out_specs, check_vma=False)
```
